16 devices in a mesh: dp: 2 (over y, z), cp: 8 (over x, core).
Axes of the slice: x: 4, y: 2, z: 1, core: 2. Of those that a mesh axis runs over, the one named last changes fastest.
The devices are a block of a 4x4x8 slice.
Arguments:
- x_act: bfloat16 [6, 1024, 5120], P('dp', 'cp'), parts along dimension 0
- d_out: bfloat16 [6, 1024, 5120], P('dp', 'cp'), parts along dimension 0
- positions: int32 [6, 1024], P('dp', 'cp'), parts along dimension 0
- ln_gain: float32 [5120], replicated
- ln_bias: float32 [5120], replicated
- w_query: bfloat16 [5120, 32, 128], replicated
- w_key: bfloat16 [5120, 8, 128], replicated
- w_value: bfloat16 [5120, 8, 128], replicated
- w_out: bfloat16 [4096, 5120], replicated
Outputs:
- output 1: bfloat16 [6, 1024, 5120], P('dp', 'cp'), parts along dimension 0
- output 2: bfloat16 [6, 1024, 5120], P('dp', 'cp'), parts along dimension 0
- output 3: float32 [10240, 32, 128], P(('dp', 'cp')), parts along dimension 0
- output 4: float32 [10240, 8, 128], P(('dp', 'cp')), parts along dimension 0
- output 5: float32 [10240, 8, 128], P(('dp', 'cp')), parts along dimension 0
- output 6: float32 [8192, 5120], P(('dp', 'cp')), parts along dimension 0
- output 7: float32 [10240], P('dp'), parts along dimension 0
- output 8: float32 [10240], P('dp'), parts along dimension 0
There are 2 independent parts. The reference program is written for one: setup_inputs(seed, part) draws one part's arguments, and reference() takes and returns one part's arrays. A program takes and returns all parts, laid end to end along the dimension named above; an argument that names none is the same for every part.
All inputs are finite; a program needn't handle non-finite values.
Results may differ from the reference program's by a relative error of at most 0.00684726.
Values are sent between devices in bfloat16 or wider.
A program may use at most 768 MiB of HBM per device.

```python
import math
import jax
import jax.numpy as jnp
from jax import lax

BATCH = 3
SEQ = 1024
WIDTH = 5120
Q_HEADS = 32
KV_HEADS = 8
HEAD_DIM = 128
Q_TILE = 128
TOKEN_KINDS = 64
DOC_SPAN = 128
GROUPS = Q_HEADS // KV_HEADS
EPS = 1e-5
ROPE_BASE = 10000.0


def setup_inputs(seed: int = 0, part: int = 0) -> dict:
    part_keys = jax.random.split(jax.random.fold_in(jax.random.key(seed), part), 5)
    shared_keys = jax.random.split(jax.random.key(seed + 1), 6)
    tokens = jax.random.randint(part_keys[0], (BATCH, SEQ), 0, TOKEN_KINDS)
    token_table = jax.random.normal(part_keys[1], (TOKEN_KINDS, WIDTH), jnp.float32)
    noise_draw = jax.random.normal(part_keys[2], (BATCH, SEQ, WIDTH), jnp.float32)
    x_act = (token_table[tokens] + 0.5 * noise_draw).astype(jnp.bfloat16)
    d_out = jax.random.normal(part_keys[3], (BATCH, SEQ, WIDTH), jnp.float32).astype(jnp.bfloat16)
    doc_flags = jax.random.randint(part_keys[4], (BATCH, SEQ), 0, DOC_SPAN) == 0
    seq_index = jnp.arange(SEQ, dtype=jnp.int32)
    starts = jnp.where(doc_flags, seq_index[None, :], 0)
    positions = (seq_index[None, :] - lax.cummax(starts, axis=1)).astype(jnp.int32)
    fan_in = WIDTH ** -0.5
    w_query = jax.random.normal(shared_keys[0], (WIDTH, Q_HEADS, HEAD_DIM), jnp.float32) * fan_in
    key_noise = jax.random.normal(shared_keys[1], (WIDTH, KV_HEADS, HEAD_DIM), jnp.float32) * fan_in
    w_key = 0.8 * w_query[:, ::GROUPS, :] + 0.6 * key_noise
    w_value = jax.random.normal(shared_keys[2], (WIDTH, KV_HEADS, HEAD_DIM), jnp.float32) * fan_in
    w_out = jax.random.normal(shared_keys[3], (Q_HEADS * HEAD_DIM, WIDTH), jnp.float32) * (Q_HEADS * HEAD_DIM) ** -0.5
    ln_gain = 0.3 * jax.random.normal(shared_keys[4], (WIDTH,), jnp.float32)
    ln_bias = 0.3 * jax.random.normal(shared_keys[5], (WIDTH,), jnp.float32)
    return {'x_act': x_act, 'd_out': d_out, 'positions': positions, 'ln_gain': ln_gain, 'ln_bias': ln_bias, 'w_query': w_query.astype(jnp.bfloat16), 'w_key': w_key.astype(jnp.bfloat16), 'w_value': w_value.astype(jnp.bfloat16), 'w_out': w_out.astype(jnp.bfloat16)}


def norm_forward(x_act, ln_gain, ln_bias):
    x_f32 = x_act.astype(jnp.float32)
    centered = x_f32 - jnp.mean(x_f32, axis=-1, keepdims=True)
    inv_std = lax.rsqrt(jnp.mean(centered * centered, axis=-1, keepdims=True) + EPS)
    x_hat = centered * inv_std
    return (x_hat * (1.0 + ln_gain) + ln_bias).astype(jnp.bfloat16), x_hat, inv_std


def norm_backward(grad_h, x_hat, inv_std, ln_gain):
    grad_hat = grad_h * (1.0 + ln_gain)
    mean_one = jnp.mean(grad_hat, axis=-1, keepdims=True)
    mean_two = jnp.mean(grad_hat * x_hat, axis=-1, keepdims=True)
    return inv_std * (grad_hat - mean_one - x_hat * mean_two)


def rope_tables(positions):
    quarter = HEAD_DIM // 4
    freq_tab = jnp.exp(jnp.arange(quarter, dtype=jnp.float32) * (-2.0 * math.log(ROPE_BASE) / (HEAD_DIM // 2)))
    angles = positions.astype(jnp.float32)[..., None] * freq_tab
    return jnp.cos(angles)[..., None, :], jnp.sin(angles)[..., None, :]


def rope_rotate(values, cos_tab, sin_tab):
    quarter = cos_tab.shape[-1]
    first_half = values[..., :quarter]
    second_half = values[..., quarter:2 * quarter]
    return jnp.concatenate([first_half * cos_tab - second_half * sin_tab, second_half * cos_tab + first_half * sin_tab, values[..., 2 * quarter:]], axis=-1)


def tile_probs(q_tile, key_f, q_first):
    scores = jnp.einsum('bqkgd,blkd->bkgql', q_tile, key_f) * (HEAD_DIM ** -0.5)
    q_index = q_first + jnp.arange(Q_TILE)
    k_index = jnp.arange(SEQ)
    scores = jnp.where(k_index[None, :] <= q_index[:, None], scores, -1e30)
    shifted = jnp.exp(scores - jnp.max(scores, axis=-1, keepdims=True))
    return shifted / jnp.sum(shifted, axis=-1, keepdims=True)


def attention_forward(q_grouped, key_f, value_f):
    def one_tile(tile_idx):
        q_first = tile_idx * Q_TILE
        q_tile = lax.dynamic_slice_in_dim(q_grouped, q_first, Q_TILE, axis=1)
        tile_prob = tile_probs(q_tile, key_f, q_first)
        prob_bf16 = tile_prob.astype(jnp.bfloat16).astype(jnp.float32)
        return jnp.einsum('bkgql,blkd->bqkgd', prob_bf16, value_f).astype(jnp.bfloat16)
    out_tiles = lax.map(one_tile, jnp.arange(SEQ // Q_TILE))
    return jnp.moveaxis(out_tiles, 0, 1).reshape(BATCH * SEQ, Q_HEADS * HEAD_DIM)


def attention_backward(q_grouped, key_f, value_f, grad_attn):
    def one_tile(acc_pair, tile_idx):
        grad_k, grad_v = acc_pair
        q_first = tile_idx * Q_TILE
        q_tile = lax.dynamic_slice_in_dim(q_grouped, q_first, Q_TILE, axis=1)
        ga_tile = lax.dynamic_slice_in_dim(grad_attn, q_first, Q_TILE, axis=1)
        tile_prob = tile_probs(q_tile, key_f, q_first)
        grad_prob = jnp.einsum('bqkgd,blkd->bkgql', ga_tile, value_f)
        row_dot = jnp.sum(tile_prob * grad_prob, axis=-1, keepdims=True)
        grad_score = (tile_prob * (grad_prob - row_dot) * (HEAD_DIM ** -0.5)).astype(jnp.bfloat16).astype(jnp.float32)
        grad_q = jnp.einsum('bkgql,blkd->bqkgd', grad_score, key_f)
        grad_k = grad_k + jnp.einsum('bkgql,bqkgd->blkd', grad_score, q_tile)
        prob_bf16 = tile_prob.astype(jnp.bfloat16).astype(jnp.float32)
        grad_v = grad_v + jnp.einsum('bkgql,bqkgd->blkd', prob_bf16, ga_tile)
        return (grad_k, grad_v), grad_q
    zero_acc = jnp.zeros((BATCH, SEQ, KV_HEADS, HEAD_DIM), jnp.float32)
    (grad_k, grad_v), q_tiles = lax.scan(one_tile, (zero_acc, zero_acc), jnp.arange(SEQ // Q_TILE))
    grad_q = jnp.moveaxis(q_tiles, 0, 1).reshape(BATCH, SEQ, Q_HEADS, HEAD_DIM)
    return grad_q, grad_k, grad_v


def reference(x_act, d_out, positions, ln_gain, ln_bias, w_query, w_key, w_value, w_out):
    n_tokens = BATCH * SEQ
    wq_flat = w_query.reshape(WIDTH, Q_HEADS * HEAD_DIM)
    wk_flat = w_key.reshape(WIDTH, KV_HEADS * HEAD_DIM)
    wv_flat = w_value.reshape(WIDTH, KV_HEADS * HEAD_DIM)
    normed, x_hat, inv_std = norm_forward(x_act, ln_gain, ln_bias)
    flat_h = normed.reshape(n_tokens, WIDTH)
    cos_tab, sin_tab = rope_tables(positions)
    q_act = rope_rotate(jnp.dot(flat_h, wq_flat, preferred_element_type=jnp.float32).reshape(BATCH, SEQ, Q_HEADS, HEAD_DIM), cos_tab, sin_tab).astype(jnp.bfloat16)
    k_act = rope_rotate(jnp.dot(flat_h, wk_flat, preferred_element_type=jnp.float32).reshape(BATCH, SEQ, KV_HEADS, HEAD_DIM), cos_tab, sin_tab).astype(jnp.bfloat16)
    v_act = jnp.dot(flat_h, wv_flat, preferred_element_type=jnp.float32).astype(jnp.bfloat16).reshape(BATCH, SEQ, KV_HEADS, HEAD_DIM)
    q_grouped = q_act.reshape(BATCH, SEQ, KV_HEADS, GROUPS, HEAD_DIM).astype(jnp.float32)
    key_f = k_act.astype(jnp.float32)
    value_f = v_act.astype(jnp.float32)
    attn_act = attention_forward(q_grouped, key_f, value_f)
    block_out = (x_act.astype(jnp.float32) + jnp.dot(attn_act, w_out, preferred_element_type=jnp.float32).reshape(BATCH, SEQ, WIDTH)).astype(jnp.bfloat16)
    grad_flat = d_out.reshape(n_tokens, WIDTH)
    grad_wo = jnp.dot(attn_act.T, grad_flat, preferred_element_type=jnp.float32)
    grad_attn = jnp.dot(grad_flat, w_out.T, preferred_element_type=jnp.float32).astype(jnp.bfloat16)
    grad_q, grad_k, grad_v = attention_backward(q_grouped, key_f, value_f, grad_attn.reshape(BATCH, SEQ, KV_HEADS, GROUPS, HEAD_DIM).astype(jnp.float32))
    grad_q_pre = rope_rotate(grad_q, cos_tab, -sin_tab).astype(jnp.bfloat16).reshape(n_tokens, Q_HEADS * HEAD_DIM)
    grad_k_pre = rope_rotate(grad_k, cos_tab, -sin_tab).astype(jnp.bfloat16).reshape(n_tokens, KV_HEADS * HEAD_DIM)
    grad_v_pre = grad_v.astype(jnp.bfloat16).reshape(n_tokens, KV_HEADS * HEAD_DIM)
    grad_h = (jnp.dot(grad_q_pre, wq_flat.T, preferred_element_type=jnp.float32) + jnp.dot(grad_k_pre, wk_flat.T, preferred_element_type=jnp.float32) + jnp.dot(grad_v_pre, wv_flat.T, preferred_element_type=jnp.float32)).reshape(BATCH, SEQ, WIDTH)
    grad_wq = jnp.dot(flat_h.T, grad_q_pre, preferred_element_type=jnp.float32).reshape(WIDTH, Q_HEADS, HEAD_DIM)
    grad_wk = jnp.dot(flat_h.T, grad_k_pre, preferred_element_type=jnp.float32).reshape(WIDTH, KV_HEADS, HEAD_DIM)
    grad_wv = jnp.dot(flat_h.T, grad_v_pre, preferred_element_type=jnp.float32).reshape(WIDTH, KV_HEADS, HEAD_DIM)
    grad_x = (d_out.astype(jnp.float32) + norm_backward(grad_h, x_hat, inv_std, ln_gain)).astype(jnp.bfloat16)
    grad_gain = jnp.sum(grad_h * x_hat, axis=(0, 1))
    grad_bias = jnp.sum(grad_h, axis=(0, 1))
    return (block_out, grad_x, grad_wq, grad_wk, grad_wv, grad_wo, grad_gain, grad_bias)
```

```python
import functools
import math
import jax
import jax.numpy as jnp
from jax import lax
from jax.experimental import pallas as pl
from jax.experimental.pallas import tpu as pltpu
from jax.sharding import PartitionSpec as P

BF, F32 = jnp.bfloat16, jnp.float32
NT = (((1,), (1,)), ((), ()))
EPS = 1e-5
VL = 67043328
ANY = pl.BlockSpec(memory_space=pl.ANY)
sds = jax.ShapeDtypeStruct
V, DS = pltpu.VMEM, pltpu.SemaphoreType.DMA


def params(**kw): return pltpu.CompilerParams(vmem_limit_bytes=VL, **kw)


def ln_stats(x):
    mean = jnp.mean(x, axis=-1, keepdims=True)
    cen = x - mean
    inv = lax.rsqrt(jnp.mean(cen * cen, axis=-1, keepdims=True) + EPS)
    return cen * inv, inv


def norm_kernel(x_ref, g_ref, c_ref, h_ref):
    x_hat, _ = ln_stats(x_ref[...].astype(F32))
    h_ref[...] = (x_hat * (1.0 + g_ref[...]) + c_ref[...]).astype(BF)


def norm_call(x, gain, bias):
    n, w = x.shape
    bm = n // 6
    row = pl.BlockSpec((1, w), lambda i: (0, 0))
    blk = pl.BlockSpec((bm, w), lambda i: (i, 0))
    return pl.pallas_call(norm_kernel, grid=(n // bm,), in_specs=[blk, row, row], out_specs=blk, out_shape=sds((n, w), BF), compiler_params=params(), name='norm')(x, gain[None], bias[None])


def out_kernel(parts, a_ref, *refs):
    w_refs, (x_ref, o_ref, lhs, sem) = refs[:parts], refs[parts:]
    nb, nk, bt, w4 = a_ref.shape

    @pl.when(pl.program_id(0) == 0)
    def _():
        cps = [pltpu.make_async_copy(a_ref.at[b, n], lhs.at[b * bt:(b + 1) * bt, n * w4:(n + 1) * w4], sem.at[b * nk + n]) for b in range(nb) for n in range(nk)]
        for cp in cps: cp.start()
        for cp in cps: cp.wait()
    kp = w_refs[0].shape[0]
    acc = x_ref[...].astype(F32)
    for k in range(parts): acc += jnp.dot(lhs[:, k * kp:(k + 1) * kp], w_refs[k][...], preferred_element_type=F32)
    o_ref[...] = acc.astype(BF)


def out_call(a_own, w_out, x, tn=512, parts=4):
    nb, nk, bt, w4 = a_own.shape
    k, w = w_out.shape
    m = nb * bt
    wspec = lambda p: pl.BlockSpec((k // parts, tn), lambda i: (p, i))
    return pl.pallas_call(functools.partial(out_kernel, parts), grid=(w // tn,), in_specs=[ANY] + [wspec(p) for p in range(parts)] + [pl.BlockSpec((m, tn), lambda i: (0, i))],
                          out_specs=pl.BlockSpec((m, tn), lambda i: (0, i)), out_shape=sds((m, w), BF), scratch_shapes=[V((m, k), BF), DS((nb * nk,))], compiler_params=params(), name='out')(a_own, *[w_out] * parts, x)


def dwo_kernel(parts, a_ref, *refs):
    dy_refs, (o_ref, lhsT) = refs[:parts], refs[parts:]

    @pl.when(pl.program_id(0) == 0)
    def _(): lhsT[...] = a_ref[...].T
    kp = dy_refs[0].shape[0]
    o_ref[...] = sum(jnp.dot(lhsT[:, k * kp:(k + 1) * kp], dy_refs[k][...], preferred_element_type=F32) for k in range(parts))


def dwo_call(a4, dy, tn=512, parts=3):
    t, m = a4.shape
    w = dy.shape[1]
    spec = lambda p: pl.BlockSpec((t // parts, tn), lambda i: (p, i))
    return pl.pallas_call(functools.partial(dwo_kernel, parts), grid=(w // tn,), in_specs=[pl.BlockSpec((t, m), lambda i: (0, 0))] + [spec(p) for p in range(parts)],
                          out_specs=pl.BlockSpec((m, tn), lambda i: (0, i)), out_shape=sds((m, w), F32), scratch_shapes=[V((m, t), BF)], compiler_params=params(), name='dwo')(a4, *[dy] * parts)


def dw_kernel(nh, h_ref, d_ref, q_ref, k_ref, v_ref, hT, hbuf, rhs, stage, sem):
    nb, nk, seq, dc = d_ref.shape
    me = lax.axis_index('cp')
    i, last = pl.program_id(0), pl.num_programs(0)
    nr = hT.shape[0]
    hd = stage.shape[3]
    per = nh * hd

    def fetch(j, slot, go):
        @pl.when(j < nk // 2)
        def _():
            for b in range(nb):
                for u in range(2):
                    cp = pltpu.make_async_copy(d_ref.at[b, 2 * jnp.minimum(j, nk // 2 - 1) + u, :, 0:per], rhs.at[slot, b * seq:(b + 1) * seq, u * per:(u + 1) * per], sem.at[slot, b * nk + u])
                    cp.start() if go else cp.wait()

        @pl.when(j >= nk // 2)
        def _():
            off = pl.multiple_of(per + (jnp.maximum(j, nk // 2) - nk // 2) * hd, hd)
            for b in range(nb):
                for n in range(nk):
                    cp = pltpu.make_async_copy(d_ref.at[b, n, :, pl.ds(off, hd)], rhs.at[slot, b * seq:(b + 1) * seq, n * hd:(n + 1) * hd], sem.at[slot, b * nk + n])
                    cp.start() if go else cp.wait()

    @pl.when(i == 0)
    def _():
        cp = pltpu.make_async_copy(h_ref.at[:, pl.ds(pl.multiple_of(me * nr, 128), nr)], hbuf, sem.at[2, 0])
        cp.start()
        fetch(0, 0, True)
        cp.wait()
        hT[...] = hbuf[...].T
    slot = i % 2

    @pl.when(i + 1 < last)
    def _(): fetch(i + 1, 1 - slot, True)
    fetch(i, slot, False)
    nq = nk // 2

    def put(j, slot, go):
        def one(ref, n, cond):
            @pl.when(cond)
            def _():
                cp = pltpu.make_async_copy(stage.at[slot], ref.at[:, pl.ds(pl.multiple_of(n * nk, nk), nk), :], sem.at[2, slot + 1])
                cp.start() if go else cp.wait()
        one(q_ref, jnp.minimum(j, nq - 1), j < nq)
        one(k_ref, 0, j == nq)
        one(v_ref, 0, j == nq + 1)

    @pl.when(i >= 2)
    def _(): put(i - 2, slot, False)
    stage[slot] = jnp.dot(hT[...], rhs[slot], preferred_element_type=F32).reshape(stage.shape[1:])
    put(i, slot, True)

    @pl.when(i == last - 1)
    def _():
        put(i - 1, 1 - slot, False)
        put(i, slot, False)


def dw_call(h, d, kv):
    nb, nk, seq, dc = d.shape
    t, w = h.shape
    nr = w // kv
    hd = dc // 6
    nq = nk // 2
    return pl.pallas_call(functools.partial(dw_kernel, 4), grid=(nq + 2,), in_specs=[ANY, ANY], out_specs=[ANY] * 3,
                          out_shape=[sds((nr, nq * nk, hd), F32)] + [sds((nr, nk, hd), F32)] * 2,
                          scratch_shapes=[V((nr, t), BF), V((t, nr), BF), V((2, t, nk * hd), BF), V((2, nr, nk, hd), F32), DS((3, nb * nk))], compiler_params=params(), name='dw')(h, d)


def dh_kernel(nt, parts, d_ref, *refs):
    w_refs, (x_any, dy_any, g_ref, dx_ref, s_ref, lhs, dh, x_ref, dy_ref, sem) = refs[:parts], refs[parts:]
    nb, nk, seq, dc = d_ref.shape
    me = lax.axis_index('cp')
    m = lhs.shape[0]
    bt = m // nb
    i = pl.program_id(0)
    tn = w_refs[0].shape[1]
    late = [pltpu.make_async_copy(x_any, x_ref, sem.at[nb * nk]), pltpu.make_async_copy(dy_any, dy_ref, sem.at[nb * nk + 1])]

    @pl.when(i == 0)
    def _():
        cps = [pltpu.make_async_copy(d_ref.at[b, n, pl.ds(pl.multiple_of(me * bt, bt), bt), :], lhs.at[b * bt:(b + 1) * bt, n * dc:(n + 1) * dc], sem.at[b * nk + n]) for b in range(nb) for n in range(nk)]
        for cp in cps + late: cp.start()
        for cp in cps: cp.wait()

    @pl.when(i < nt)
    def _():
        w = jnp.concatenate([r[k] for r in w_refs for k in range(r.shape[0])], axis=1)
        dh[jnp.minimum(i, nt - 1)] = lax.dot_general(lhs[...], w, NT, preferred_element_type=F32)

    @pl.when(i == nt)
    def _():
        for cp in late: cp.wait()
        s_ref[...] = jnp.zeros_like(s_ref)
        rc = 32
        sub = s_ref.shape[0] // 2
        fold = lambda v: v.reshape(rc // sub, sub, -1).sum(0)

        def body(r, _):
            rr = pl.ds(pl.multiple_of(r * rc, rc), rc)
            x_hat, inv = ln_stats(x_ref[rr, :].astype(F32))
            g = jnp.concatenate([dh[k, rr, :] for k in range(nt)], axis=1)
            gh = g * (1.0 + g_ref[...])
            m1 = jnp.mean(gh, axis=-1, keepdims=True)
            m2 = jnp.mean(gh * x_hat, axis=-1, keepdims=True)
            dx_ref[rr, :] = (dy_ref[rr, :].astype(F32) + inv * (gh - m1 - x_hat * m2)).astype(BF)
            s_ref[0:sub, :] += fold(g * x_hat)
            s_ref[sub:, :] += fold(g)
            return 0
        lax.fori_loop(0, m // rc, body, 0)


def dh_call(d, w2, x, dy, gain, tn=256, parts=3):
    nb, nk, seq, dc = d.shape
    nw, w, tw = w2.shape
    m = x.shape[0]
    nt = w // tn
    wspec = lambda p: pl.BlockSpec((nw // parts, tn, tw), lambda i: (p, jnp.minimum(i, nt - 1), 0))
    return pl.pallas_call(functools.partial(dh_kernel, nt, parts), grid=(nt + 1,), in_specs=[ANY] + [wspec(p) for p in range(parts)] + [ANY, ANY, pl.BlockSpec((1, w), lambda i: (0, 0))],
                          out_specs=[pl.BlockSpec((m, w), lambda i: (0, 0)), pl.BlockSpec((16, w), lambda i: (0, 0))], out_shape=[sds((m, w), BF), sds((16, w), F32)],
                          scratch_shapes=[V((m, nk * dc), BF), V((nt, m, tn), F32), V((m, w), BF), V((m, w), BF), DS((nb * nk + 2,))], compiler_params=params(), name='dh')(d, *[w2] * parts, x, dy, gain[None])


def sum_kernel(ncp, s_ref, o_ref, own, buf, send, recv):
    me = lax.axis_index('cp')
    M = pl.DeviceIdType.MESH
    sub = s_ref.shape[0] // 2
    barrier = pltpu.get_barrier_semaphore()
    for k in range(1, ncp): pl.semaphore_signal(barrier, inc=1, device_id={'cp': (me + k) % ncp}, device_id_type=M)
    for r in (0, 1): own[r:r + 1, :] = jnp.sum(s_ref[r * sub:(r + 1) * sub, :], axis=0, keepdims=True)
    pl.semaphore_wait(barrier, ncp - 1)
    cps = [pltpu.make_async_remote_copy(src_ref=own, dst_ref=buf.at[k], send_sem=send.at[k], recv_sem=recv.at[k], device_id={'cp': (me + k) % ncp}, device_id_type=M) for k in range(1, ncp)]
    for cp in cps: cp.start()
    buf[0] = own[...]
    for cp in cps: cp.wait()
    tot = buf[me]
    for dev in range(1, ncp): tot = tot + buf[(me + ncp - dev) % ncp]
    o_ref[...] = tot


def sum_call(s, ncp, cid):
    full = pl.BlockSpec(memory_space=pltpu.VMEM)
    w = s.shape[1]
    return pl.pallas_call(functools.partial(sum_kernel, ncp), in_specs=[full], out_specs=full, out_shape=sds((2, w), F32),
                          scratch_shapes=[V((2, w), F32), V((ncp, 2, w), F32), DS((ncp,)), DS((ncp,))], compiler_params=pltpu.CompilerParams(collective_id=cid, has_side_effects=True), name='sums')(s)


MASK = -1e30
HD, GQ, QB, HALF = 128, 4, 128, 64
ROT = HALF // 2
QW = GQ * HD
TW = 2 * HD
NCH = 4
UT = 3
SLOTS, RSLOTS = 4, 10
CHUNK = 2
MESH = pl.DeviceIdType.MESH


def rot(x, c, s):
    lane = lax.broadcasted_iota(jnp.int32, x.shape, 1)
    return x * c + jnp.where(lane < ROT, pltpu.roll(x, HD - ROT, 1), pltpu.roll(x, ROT, 1)) * s


def dot(a, b): return jnp.dot(a, b, preferred_element_type=F32)


def ntdot(a, b): return lax.dot_general(a, b, NT, preferred_element_type=F32)


def att_scores(i, q_ref, k_ref, v_ref, da_ref):
    L = QB * (i + 1)
    stack = lambda ref: jnp.concatenate([ref[L - QB:L, HD * h:HD * h + HD] for h in range(GQ)], axis=0)
    q4, da4 = stack(q_ref), stack(da_ref)
    return q4, da4, ntdot(k_ref[0:L, :], q4), ntdot(v_ref[0:L, :], da4)


def att_probs(i, q4, da4, sT, dpT):
    L, scale = QB * (i + 1), HD ** -0.5
    kr = lax.broadcasted_iota(jnp.int32, (QB, GQ * QB), 0)
    qc = lax.broadcasted_iota(jnp.int32, (QB, GQ * QB), 1) & (QB - 1)
    diag = jnp.where(kr <= qc, sT[L - QB:L, :], MASK)
    sT = jnp.concatenate([sT[:L - QB, :], diag], axis=0) if i else diag
    e = jnp.exp2((sT - jnp.max(sT, axis=0, keepdims=True)) * (scale * math.log2(math.e)))
    p = e * (1.0 / jnp.sum(e, axis=0, keepdims=True))
    ds = (p * (dpT - jnp.sum(p * dpT, axis=0, keepdims=True)) * scale).astype(BF)
    return q4, da4, p.astype(BF), ds


def att_store(i, kT, vT, rope, a_ref, d_ref, dk_acc, dv_acc, q4, da4, pb, ds):
    L = QB * (i + 1)
    r, full, head = slice(L - QB, L), slice(0, L), lambda h: slice(HD * h, HD * h + HD)
    aT = dot(vT[:, full], pb)
    for h in range(GQ): a_ref[r, head(h)] = aT[:, head(h)].T.astype(BF)
    dv_acc[full, :] += dot(pb, da4)
    dk_acc[full, :] += dot(ds, q4)
    dqT = dot(kT[:, full], ds)
    c, s = rope[0, r, :], -rope[1, r, :]
    for h in range(GQ): d_ref[r, head(h)] = rot(dqT[:, head(h)].T, c, s).astype(BF)


def kg_kernel(nchip, owned, plan, h_own, dy_own, cs_own, wq, wk, wv, wo,
              h_all, dy_all, w2, a_own, a4, dqkv, cs_all, q_hbm, k_hbm, v_hbm, da_hbm, a_tmp,
              lhs, rope,
              send, recv, csend, crecv, wsend, wrecv, rsend, rrecv, osend, orecv, asend, arecv, fsend, frecv,
              lsem, wsem, osem, isem, iosem, aisem, aosem, ownsem, bsem):
    nb, bt, width = h_own.shape
    nkv = w2.shape[0] // UT
    T = q_hbm.shape[2]
    nloc = nkv // 2
    cb = 2 * bt
    me = lax.axis_index('cp')
    chip, core = me // 2, me % 2
    at = lambda step, c=core: 2 * ((chip + step) % nchip) + c
    right, left, opp, part = at(1), at(nchip - 1), at(2), 2 * chip + 1 - core
    other = 1 - core
    own_t, all_t = (h_own, dy_own), (h_all, dy_all)
    ds = lambda i, n: pl.ds(pl.multiple_of(i * n, n), n)
    blk = lambda a: ds(a, bt)

    barrier = pltpu.get_barrier_semaphore()
    ncp = 2 * nchip
    for k in range(1, ncp): pl.semaphore_signal(barrier, inc=1, device_id={'cp': (me + k) % ncp}, device_id_type=MESH)
    pl.semaphore_wait(barrier, ncp - 1)

    def remote(src, dst, s, r, dev):
        return pltpu.make_async_remote_copy(src_ref=src, dst_ref=dst, send_sem=s, recv_sem=r, device_id={'cp': dev}, device_id_type=MESH)

    local = pltpu.make_async_copy
    pending = []

    def go(make, *ar):
        make(*ar).start()
        pending.append((make, ar))

    def ring(view, own, ss, rs, half):
        def copy(ch, src, slot, dev, lo=0, n=2 * half): return remote(src if src is not None else view(slot, lo, n), view(slot, lo, n), ss.at[ch], rs.at[ch], dev)

        def D():
            for ch, dev in enumerate((right, left, part)): go(copy, ch, own, me, dev)

        def got(ch, slot, lo=0, n=2 * half): copy(ch, None, slot, part, lo, n).wait_recv()

        def Fw():
            got(0, left)
            go(copy, 3, None, left, right, 0, half)
            got(1, right)
            go(copy, 4, None, right, left, half, half)
            go(copy, 5, None, left, part)
            go(copy, 6, None, right, part)

        def G():
            got(3, opp, 0, half)
            got(4, opp, half, half)
            go(copy, 7, None, opp, part)

        def ready(pos):
            if pos == 0: got(2, part)
            if pos == 1: got(6, at(1, other))
            if pos == 2: got(5, at(nchip - 1, other))
            if pos == 3: got(7, at(2, other))
        return D, Fw, G, ready

    rings = []
    for t in range(2 * nb):
        b, kind = t // 2, t % 2
        view = lambda slot, lo, n, b=b, kind=kind: all_t[kind].at[b, pl.ds(pl.multiple_of(slot * bt + lo, bt // 2), n), :]
        rings.append(ring(view, own_t[kind].at[b], send.at[t], recv.at[t], bt // 2))
    oview = lambda slot, lo, n: dqkv.at[owned, slot, pl.ds(lo, n), :]
    rings.append(ring(oview, dqkv.at[owned, me], osend, orecv, q_hbm.shape[2] // 2))

    def cs_copy(b, ch, src, slot, dev): return remote(src, cs_all.at[b, blk(slot), :], csend.at[b, ch], crecv.at[b, ch], dev)

    def cs_send(b):
        for ch, dev in enumerate((right, opp, left, part)): go(cs_copy, b, ch, cs_own.at[b], me, dev)

    def cs_forward(b):
        for ch, slot in enumerate((left, opp, right)):
            cs_copy(b, ch, cs_own.at[b], slot, part).wait_recv()
            go(cs_copy, b, 4 + ch, cs_all.at[b, blk(slot), :], slot, part)

    def cs_ready(b):
        cs_copy(b, 3, cs_own.at[b], part, part).wait_recv()
        for ch, step in enumerate((nchip - 1, 2, 1)): cs_copy(b, 4 + ch, cs_own.at[b], at(step, other), part).wait_recv()

        def scope(cst):
            for dev in range(ncp):
                @pl.when(dev != me)
                def _(): local(cs_all.at[b, dev * bt:(dev + 1) * bt, :], cst.at[dev * bt:(dev + 1) * bt, :], bsem.at[dev]).start()
            local(cs_own.at[b], cst.at[blk(me), :], bsem.at[me]).start()
            for dev in range(ncp): local(cs_own.at[b], cst.at[dev * bt:(dev + 1) * bt, :], bsem.at[dev]).wait()
            packed = cst[...]
            turned = lax.broadcasted_iota(jnp.int32, packed.shape, 1) < HALF
            rope[b, 0] = jnp.where(turned, packed, 1.0)
            rope[b, 1] = jnp.where(turned, pltpu.roll(packed, HALF, 1), 0.0)
        pl.run_scoped(scope, V((T, HD), F32))

    STEP = (0, 1, nchip - 1, 2)
    crow = lambda pos: ds((chip + STEP[pos]) % nchip, cb)

    def loads(t, pos):
        b, kind = t // 2, t % 2
        if pos == 0:
            return [local(own_t[kind].at[b], lhs.at[kind, blk(core), :], lsem.at[kind, 0]), local(all_t[kind].at[b, blk(part), :], lhs.at[kind, blk(other), :], lsem.at[kind, nchip])]
        return [local(all_t[kind].at[b, crow(pos), :], lhs.at[kind, pl.ds(pos * cb, cb), :], lsem.at[kind, pos])]

    def own_back(t): return local(lhs.at[t % 2, blk(core), :], all_t[t % 2].at[t // 2, blk(me), :], ownsem.at[t % 2])

    def load(t, pos_list):
        for pos in pos_list:
            rings[t][3](pos)
            for cp in loads(t, pos): cp.start()

    def key_head(b, i): return me if b == owned else 2 * mine(i // 2) + i % 2

    def tiles(t, pos_list, per, shape, start, wait, compute, dst, mid):
        b, kind = t // 2, t % 2
        m0, m = pos_list[0] * cb, len(pos_list) * cb
        cnt = per * (1 if b == owned else nloc)
        tid = lambda x: per * key_head(b, x // per) + x % per

        def scope(buf, ost):
            for x in range(min(cnt, SLOTS)): start(tid(x), buf, x)
            for pos in pos_list:
                for cp in loads(t, pos): cp.wait()
            if pos_list[0] == 0: own_back(t).start()

            def stores(x, slot, start_it):
                for y, pos in enumerate(pos_list):
                    dst(b, x // per, x % per, crow(pos), ost.at[slot, pl.ds(y * cb, cb), :], slot, y, start_it)

            def body(x, _):
                for when, ops in mid.items():
                    @pl.when(x == when)
                    def _():
                        for op, *ar in ops: ACT[op](*ar)
                slot, ws = x % 2, x % SLOTS
                wait(tid(x), buf, ws)

                @pl.when(x >= 1)
                def _():
                    @pl.when(x + SLOTS - 1 < cnt)
                    def _(): start(tid(x + SLOTS - 1), buf, (x + SLOTS - 1) % SLOTS)

                @pl.when(x >= 2)
                def _(): stores(x - 2, slot, False)
                compute(b, x % per, lambda r, n: lhs[kind, m0 + r:m0 + r + n, :], buf.at[ws], ost, slot, pos_list)
                stores(x, slot, True)
                return 0
            lax.fori_loop(0, cnt, body, 0)
            for x in (cnt - 2, cnt - 1): stores(x, x % 2, False)
            if pos_list[0] == 0: own_back(t).wait()
        pl.run_scoped(scope, V((SLOTS,) + shape, BF), V((2, m, TW), BF))

    def run(cp, start_it): cp.start() if start_it else cp.wait()

    def w_start(n, buf, slot):
        c = width // NCH
        for y in range(NCH): local(w2.at[n, pl.ds(y * c, c), :], buf.at[slot, pl.ds(y * c, c), :], wsem.at[slot]).start()

    def w_wait(n, buf, slot): local(w2.at[n], buf.at[slot], wsem.at[slot]).wait()

    def qkv_dst(b, i, u, rr, src, slot, y, start_it):
        @pl.when(u < 2)
        def _(): run(local(src, q_hbm.at[b, i, rr, ds(jnp.minimum(u, 1), TW)], osem.at[slot, y]), start_it)

        @pl.when(u == 2)
        def _():
            run(local(src.at[:, 0:HD], k_hbm.at[b, i, rr, :], osem.at[slot, y]), start_it)
            run(local(src.at[:, HD:TW], v_hbm.at[b, i, rr, :], osem.at[slot, nchip + y]), start_it)

    def qkv_compute(b, u, left, w, ost, slot, pos_list):
        for y0 in range(0, len(pos_list), CHUNK):
            part_list = pos_list[y0:y0 + CHUNK]
            res = dot(left(y0 * cb, len(part_list) * cb), w[...])
            for y, pos in enumerate(part_list):
                c, s = rope[b, 0, crow(pos), :], rope[b, 1, crow(pos), :]
                rr, ro = slice(y * cb, (y + 1) * cb), slice((y0 + y) * cb, (y0 + y + 1) * cb)
                ost[slot, ro, 0:HD] = rot(res[rr, 0:HD], c, s).astype(BF)
                ost[slot, ro, HD:TW] = jnp.where(u == 2, res[rr, HD:TW], rot(res[rr, HD:TW], c, s)).astype(BF)

    def qkv(b, pos_list, mid={}): tiles(2 * b, pos_list, UT, (width, TW), w_start, w_wait, qkv_compute, qkv_dst, mid)

    def o_start(n, buf, slot):
        c = TW // NCH
        for y in range(NCH): local(wo.at[ds(n * NCH + y, c), :], buf.at[slot, pl.ds(y * c, c), :], wsem.at[slot]).start()

    def o_wait(n, buf, slot): local(wo.at[ds(n, TW), :], buf.at[slot], wsem.at[slot]).wait()

    def da_dst(b, i, u, rr, src, slot, y, start_it): run(local(src, da_hbm.at[b, i, rr, ds(u, TW)], osem.at[slot, y]), start_it)

    def da_compute(b, u, left, w, ost, slot, pos_list):
        for y0 in range(0, len(pos_list), CHUNK):
            n = min(CHUNK, len(pos_list) - y0) * cb
            ost[slot, y0 * cb:y0 * cb + n, :] = ntdot(left(y0 * cb, n), w[...]).astype(BF)

    def da(b, pos_list, mid={}): tiles(2 * b + 1, pos_list, 2, (TW, width), o_start, o_wait, da_compute, da_dst, mid)

    OCT = nkv

    def rl(src_of, dst_of, nblk):
        def scope(wst, wrl):
            for i in range(RSLOTS): src_of(i, wst.at[i], i).start()

            def body(j, _):
                for u in range(RSLOTS):
                    i, slot = RSLOTS * j + u, u % 2
                    src_of(i, wst.at[u], u).wait()

                    @pl.when(i >= 2)
                    def _():
                        for cp in dst_of(i - 2, wrl.at[slot], slot): cp.wait()
                    wrl[slot] = wst[u].reshape(RB, OCT * HD)
                    for cp in dst_of(i, wrl.at[slot], slot): cp.start()

                    @pl.when(i + RSLOTS < nblk)
                    def _(): src_of(i + RSLOTS, wst.at[u], u).start()
                return 0
            lax.fori_loop(0, nblk // RSLOTS, body, 0)
            for slot in (0, 1):
                for cp in dst_of(nblk - 2 + slot, wrl.at[slot], slot): cp.wait()
        pl.run_scoped(scope, V((RSLOTS, RB, OCT, HD), BF), V((2, RB, OCT * HD), BF))

    half_w = width // 2
    mine = lambda t: t * 2 + core
    theirs = lambda t: t * 2 + other

    def q_tile(octet, x): return UT * (2 * octet + x // 2) + x % 2

    def w_copy(ch, tile, rows): return remote(w2.at[tile, rows, :], w2.at[tile, rows, :], wsend.at[ch], wrecv.at[ch], part)

    def rl_q(t):
        rl(lambda i, buf, slot: local(wq.at[ds(i, RB), ds(mine(t), OCT), :], buf, isem.at[slot]),
           lambda i, buf, slot: [local(buf.at[:, pl.ds(TW * x, TW)], w2.at[q_tile(mine(t), x), ds(i, RB), :], iosem.at[slot, x]) for x in range(NCH)], width // RB)

    def q_copy(t, x): return w_copy(t * NCH + x, q_tile(mine(t), x), pl.ds(0, width))

    def q_send(t):
        for x in range(NCH): go(q_copy, t, x)

    def rl_kv(kv):
        w = (wk, wv)[kv]
        base = half_w // RB
        rl(lambda i, buf, slot: local(w.at[ds(core * base + i, RB)], buf, isem.at[slot]),
           lambda i, buf, slot: [local(buf.at[:, pl.ds(n * HD, HD)], w2.at[UT * n + 2, ds(core * base + i, RB), kv * HD:(kv + 1) * HD], iosem.at[slot, n]) for n in range(nkv)], base)
        if kv:
            for n in range(nkv): go(w_copy, 2 * NCH + n, UT * n + 2, ds(core, half_w))

    def wq_ready():
        for t in (0, 1):
            for x in range(NCH): w_copy(t * NCH + x, q_tile(theirs(t), x), pl.ds(0, width)).wait_recv()

    def wkv_ready():
        for n in range(nkv): w_copy(2 * NCH + n, UT * n + 2, ds(other, half_w)).wait_recv()

    def att_ins(b, i, slot, bufs): return [local(src.at[b, i], dst.at[slot], aisem.at[slot, x]) for x, (src, dst) in enumerate(zip((q_hbm, k_hbm, v_hbm, da_hbm), bufs))]

    def att_outs(b, i, slot, out_a, out_d):
        n = key_head(b, i)
        return [local(out_a.at[slot], a_tmp.at[b, i], aosem.at[slot, 0]), local(out_d.at[slot], dqkv.at[b, n], aosem.at[slot, 1]), local(out_a.at[slot, blk(me), :], a_own.at[b, n], aosem.at[slot, 2])]

    def keep(b, i, slot, out_a, start_it):
        @pl.when(key_head(b, i) == me)
        def _(): run(local(out_a.at[slot], a4.at[b], aosem.at[slot, 3]), start_it)

    whole = [b for b in range(nb) if b != owned]

    def pair_copies(b, i, n):
        f = whole.index(b)
        return [remote(dqkv.at[b, n], dqkv.at[b, n], rsend.at[f, i, 0], rrecv.at[f, i, 0], part),
                remote(a_tmp.at[b, i, blk(part), :], a_own.at[b, n], rsend.at[f, i, 1], rrecv.at[f, i, 1], part)]

    def four_copy(b, i): return remote(a_tmp.at[b, i], a4.at[b], fsend.at[whole.index(b)], frecv.at[whole.index(b)], part)

    def att(b):
        cnt = 1 if b == owned else nloc

        def scope(in_q, in_k, in_v, in_da, out_a, out_d, dk_acc, dv_acc, kT, vT):
            bufs = (in_q, in_k, in_v, in_da)
            for cp in att_ins(b, 0, 0, bufs): cp.start()

            def done(i, slot):
                for cp in att_outs(b, i, slot, out_a, out_d): cp.wait()
                keep(b, i, slot, out_a, False)
                if b != owned:
                    for cp in pair_copies(b, i, key_head(b, i)): cp.start()

                    @pl.when(key_head(b, i) == part)
                    def _(): four_copy(b, i).start()

            def body(i, _):
                slot = i % 2
                for cp in att_ins(b, i, slot, bufs): cp.wait()

                @pl.when(i + 1 < cnt)
                def _():
                    for cp in att_ins(b, i + 1, 1 - slot, bufs): cp.start()

                @pl.when(i >= 2)
                def _(): done(i - 2, slot)
                hook(b, i)
                q, k, v, g = (r.at[slot] for r in bufs)
                dk_acc[...] = jnp.zeros_like(dk_acc)
                dv_acc[...] = jnp.zeros_like(dv_acc)
                kT[...] = k[...].T
                vT[...] = v[...].T
                nblk = T // QB
                scores = att_scores(0, q, k, v, g)
                for x in range(nblk):
                    following = att_scores(x + 1, q, k, v, g) if x + 1 < nblk else None
                    att_store(x, kT, vT, rope.at[b], out_a.at[slot], out_d.at[slot], dk_acc, dv_acc, *att_probs(x, *scores))
                    scores = following
                out_d[slot, :, QW:QW + HD] = rot(dk_acc[...], rope[b, 0], -rope[b, 1]).astype(BF)
                out_d[slot, :, QW + HD:] = dv_acc[...].astype(BF)
                for cp in att_outs(b, i, slot, out_a, out_d): cp.start()
                keep(b, i, slot, out_a, True)
                return 0
            lax.fori_loop(0, cnt, body, 0)
            for i in range(max(cnt - 2, 0), cnt): done(i, i % 2)
        two = lambda w: V((2, T, w), BF)
        pl.run_scoped(scope, two(QW), two(HD), two(HD), two(QW), two(QW), two(QW + TW), V((T, HD), F32), V((T, HD), F32), V((HD, T), BF), V((HD, T), BF))

    hooks = {}

    def hook(b, i):
        for j, ops in hooks.get(b, {}).items():
            @pl.when(i == j)
            def _():
                for op, *ar in ops: ACT[op](*ar)

    def a_copy(k, src, slot, dev): return remote(src, a_own.at[owned, slot], asend.at[k], arecv.at[k], dev)

    def a_send():
        for k in range(1, ncp): go(a_copy, k, a_tmp.at[owned, 0, blk((me + k) % ncp), :], me, (me + k) % ncp)

    def all_in():
        for k in range(1, ncp): a_copy(k, a_tmp.at[owned, 0, blk(me), :], (me + ncp - k) % ncp, part).wait_recv()
        for b in whole:
            for i in range(nloc):
                for cp in pair_copies(b, i, key_head(b, i)): cp.wait_send()
                for cp in pair_copies(b, i, 2 * theirs(i // 2) + i % 2): cp.wait_recv()

            @pl.when(chip % 2 == core)
            def _(): four_copy(b, 0).wait_send()

            @pl.when(chip % 2 != core)
            def _(): four_copy(b, 0).wait_recv()

    ACT = {'L0': lambda t, ps: [cp.start() for p in ps for cp in loads(t, p)], 'T': cs_send, 'TF': cs_forward, 'TR': cs_ready, 'D': lambda t: rings[t][0](), 'F': lambda t: rings[t][1](), 'G': lambda t: rings[t][2](), 'N': lambda t, ps: [rings[t][3](p) for p in ps],
           'L': load, 'RQ': rl_q, 'SQ': q_send, 'RK': rl_kv, 'WQ': wq_ready, 'WK': wkv_ready, 'Q': qkv, 'O': da, 'AS': a_send, 'IN': all_in, 'H': lambda b, j, ops: hooks.setdefault(b, {}).update({j: ops}), 'A': att}
    for op, *ar in plan: ACT[op](*ar)
    for make, ar in pending: make(*ar).wait_send()


S0, S1, S2, S3, S4, S5, S6, S7, S8, S9, S10 = range(11)
NEAR, FAR, EACH, HERE, AWAY = (S0, S1, S2), (S3,), (S0, S1, S2, S3), (S0,), (S1, S2, S3)
PLAN = [('T', S0), ('D', S0), ('D', S1), ('T', S1), ('T', S2), ('RK', S0), ('RK', S1), ('RQ', S0), ('TF', S0), ('F', S0), ('D', S2), ('RQ', S1), ('TR', S0), ('L', S0, NEAR), ('WK',),
        ('Q', S0, NEAR, {S2: [('SQ', S0)], S6: [('F', S1), ('D', S3)], S10: [('L', S1, NEAR)]}), ('G', S0), ('L', S0, FAR), ('SQ', S1), ('O', S0, NEAR), ('TF', S1), ('TF', S2), ('Q', S0, FAR),
        ('F', S2), ('D', S4), ('G', S1), ('L', S1, FAR), ('TR', S1), ('TR', S2), ('L', S2, NEAR), ('O', S0, FAR),
        ('H', S0, S1, [('F', S3), ('D', S5)]), ('H', S0, S2, [('L', S3, NEAR), ('G', S2), ('L', S2, FAR)]), ('A', S0), ('WQ',),
        ('Q', S1, EACH), ('L', S4, HERE), ('F', S4), ('Q', S2, HERE), ('G', S3), ('L', S3, FAR), ('L', S4, NEAR[S1:]), ('O', S1, EACH), ('L', S5, HERE), ('A', S1),
        ('F', S5), ('D', S6), ('AS',), ('G', S4), ('L', S4, FAR), ('L', S5, NEAR[S1:]), ('Q', S2, AWAY, {S9: [('G', S5), ('L', S5, FAR)]}), ('O', S2, EACH), ('H', S2, S1, [('F', S6)]), ('H', S2, S3, [('G', S6)]), ('A', S2), ('N', S6, EACH), ('IN',)]
RB = 128


def kg_call(h_own, dy_own, cs_own, wq, wk, wv, wo, ncp, owned=1, plan=None):
    nb, bt, width = h_own.shape
    T = bt * ncp
    nkv = wk.shape[1]
    nloc = nkv // 2
    seqs = lambda *s: sds((nb,) + s, BF)
    outs = [seqs(T, width)] * 2 + [sds((UT * nkv, width, TW), BF), seqs(nkv, bt, QW), seqs(T, QW), seqs(nkv, T, QW + TW), sds((nb, T, HD), F32),
            seqs(nloc, T, QW), seqs(nloc, T, HD), seqs(nloc, T, HD), seqs(nloc, T, QW), seqs(nloc, T, QW)]
    two = lambda *s: [DS(s), DS(s)]
    scratch = [V((2, T, width), BF), V((nb, 2, T, HD), F32)] + two(2 * nb, 8) + two(nb, 7) + two(2 * NCH + nkv) + two(nb - 1, nloc, 2) + two(8) + two(ncp) + two(nb - 1)
    scratch += [DS((2, 5)), DS((SLOTS,)), DS((2, 8)), DS((RSLOTS,)), DS((2, 8)), DS((2, 4)), DS((2, 4)), DS((2,)), DS((ncp,))]
    return pl.pallas_call(functools.partial(kg_kernel, ncp // 2, owned, plan or PLAN), out_shape=outs, in_specs=[ANY] * 7, out_specs=[ANY] * len(outs), scratch_shapes=scratch,
                          compiler_params=params(collective_id=0, has_side_effects=True), name='gather')(h_own, dy_own, cs_own, wq, wk, wv, wo)


ROPE_BASE = 10000.0


def rope_table(positions):
    freq_tab = jnp.exp(jnp.arange(ROT, dtype=F32) * (-2.0 * math.log(ROPE_BASE) / HALF))
    angles = positions.astype(F32)[..., None] * freq_tab
    cos, sin = jnp.cos(angles), jnp.sin(angles)
    return jnp.concatenate([cos, cos, -sin, sin], -1)


def solution(mesh):
    ncp = mesh.shape['cp']

    def device_step(x_act, d_out, positions, ln_gain, ln_bias, w_query, w_key, w_value, w_out):
        nb, bt, width = x_act.shape
        flat = lambda v: v.reshape(nb * v.shape[1], v.shape[2])
        x, dy = flat(x_act), flat(d_out)
        h = norm_call(x, ln_gain, ln_bias).reshape(x_act.shape)
        h_all, dy_all, w2, a_own, a4, dqkv = kg_call(h, d_out, rope_table(positions), w_query, w_key, w_value, w_out, ncp)[:6]
        dx, sums = dh_call(dqkv, w2, x, dy, ln_gain)
        sums = sum_call(sums, ncp, 1)
        block_out = out_call(a_own, w_out, x)
        dwo = dwo_call(flat(a4), flat(dy_all))
        dwq, dwk, dwv = dw_call(flat(h_all), dqkv, ncp)
        return (block_out.reshape(x_act.shape), dx.reshape(x_act.shape), dwq, dwk, dwv, dwo, sums[0], sums[1])

    row, rep = P('dp', 'cp', None), P(None)
    wrow = P(('dp', 'cp'), None, None)
    return jax.shard_map(device_step, mesh=mesh, in_specs=(row, row, P('dp', 'cp'), rep, rep, rep, rep, rep, rep),
                         out_specs=(row, row, wrow, wrow, wrow, P(('dp', 'cp'), None), P('dp'), P('dp')), check_vma=False)
```

```python
import functools
import math
import jax
import jax.numpy as jnp
from jax import lax
from jax.experimental import pallas as pl
from jax.experimental.pallas import tpu as pltpu
from jax.sharding import PartitionSpec as P

BF, F32 = jnp.bfloat16, jnp.float32
NT = (((1,), (1,)), ((), ()))
EPS = 1e-5
VL = 67043328
ANY = pl.BlockSpec(memory_space=pl.ANY)
sds = jax.ShapeDtypeStruct
V, DS = pltpu.VMEM, pltpu.SemaphoreType.DMA


def params(**kw): return pltpu.CompilerParams(vmem_limit_bytes=VL, **kw)


def ln_stats(x):
    mean = jnp.mean(x, axis=-1, keepdims=True)
    cen = x - mean
    inv = lax.rsqrt(jnp.mean(cen * cen, axis=-1, keepdims=True) + EPS)
    return cen * inv, inv


def norm_kernel(x_ref, g_ref, c_ref, h_ref):
    x_hat, _ = ln_stats(x_ref[...].astype(F32))
    h_ref[...] = (x_hat * (1.0 + g_ref[...]) + c_ref[...]).astype(BF)


def norm_call(x, gain, bias):
    n, w = x.shape
    bm = n // 3
    row = pl.BlockSpec((1, w), lambda i: (0, 0))
    blk = pl.BlockSpec((bm, w), lambda i: (i, 0))
    return pl.pallas_call(norm_kernel, grid=(n // bm,), in_specs=[blk, row, row], out_specs=blk, out_shape=sds((n, w), BF), compiler_params=params(), name='norm')(x, gain[None], bias[None])


def out_kernel(parts, a_ref, *refs):
    w_refs, (x_ref, o_ref, lhs, sem) = refs[:parts], refs[parts:]
    nb, nk, bt, w4 = a_ref.shape

    @pl.when(pl.program_id(0) == 0)
    def _():
        cps = [pltpu.make_async_copy(a_ref.at[b, n], lhs.at[b * bt:(b + 1) * bt, n * w4:(n + 1) * w4], sem.at[b * nk + n]) for b in range(nb) for n in range(nk)]
        for cp in cps: cp.start()
        for cp in cps: cp.wait()
    kp = w_refs[0].shape[0]
    acc = x_ref[...].astype(F32)
    for k in range(parts): acc += jnp.dot(lhs[:, k * kp:(k + 1) * kp], w_refs[k][...], preferred_element_type=F32)
    o_ref[...] = acc.astype(BF)


def out_call(a_own, w_out, x, tn=512, parts=4):
    nb, nk, bt, w4 = a_own.shape
    k, w = w_out.shape
    m = nb * bt
    wspec = lambda p: pl.BlockSpec((k // parts, tn), lambda i: (p, i))
    return pl.pallas_call(functools.partial(out_kernel, parts), grid=(w // tn,), in_specs=[ANY] + [wspec(p) for p in range(parts)] + [pl.BlockSpec((m, tn), lambda i: (0, i))],
                          out_specs=pl.BlockSpec((m, tn), lambda i: (0, i)), out_shape=sds((m, w), BF), scratch_shapes=[V((m, k), BF), DS((nb * nk,))], compiler_params=params(), name='out')(a_own, *[w_out] * parts, x)


def dwo_kernel(parts, a_ref, *refs):
    dy_refs, (o_ref, lhsT) = refs[:parts], refs[parts:]

    @pl.when(pl.program_id(0) == 0)
    def _(): lhsT[...] = a_ref[...].T
    kp = dy_refs[0].shape[0]
    o_ref[...] = sum(jnp.dot(lhsT[:, k * kp:(k + 1) * kp], dy_refs[k][...], preferred_element_type=F32) for k in range(parts))


def dwo_call(a4, dy, tn=1024, parts=3):
    t, m = a4.shape
    w = dy.shape[1]
    spec = lambda p: pl.BlockSpec((t // parts, tn), lambda i: (p, i))
    return pl.pallas_call(functools.partial(dwo_kernel, parts), grid=(w // tn,), in_specs=[pl.BlockSpec((t, m), lambda i: (0, 0))] + [spec(p) for p in range(parts)],
                          out_specs=pl.BlockSpec((m, tn), lambda i: (0, i)), out_shape=sds((m, w), F32), scratch_shapes=[V((m, t), BF)], compiler_params=params(), name='dwo')(a4, *[dy] * parts)


def dw_kernel(nh, h_ref, d_ref, q_ref, k_ref, v_ref, hT, hbuf, rhs, stage, sem):
    nb, nk, seq, dc = d_ref.shape
    me = lax.axis_index('cp')
    i, last = pl.program_id(0), pl.num_programs(0)
    nr = hT.shape[0]
    hd = stage.shape[3]
    per = nh * hd

    def fetch(j, slot, go):
        @pl.when(j < nk // 2)
        def _():
            for b in range(nb):
                for u in range(2):
                    cp = pltpu.make_async_copy(d_ref.at[b, 2 * jnp.minimum(j, nk // 2 - 1) + u, :, 0:per], rhs.at[slot, b * seq:(b + 1) * seq, u * per:(u + 1) * per], sem.at[slot, b * nk + u])
                    cp.start() if go else cp.wait()

        @pl.when(j >= nk // 2)
        def _():
            off = pl.multiple_of(per + (jnp.maximum(j, nk // 2) - nk // 2) * hd, hd)
            for b in range(nb):
                for n in range(nk):
                    cp = pltpu.make_async_copy(d_ref.at[b, n, :, pl.ds(off, hd)], rhs.at[slot, b * seq:(b + 1) * seq, n * hd:(n + 1) * hd], sem.at[slot, b * nk + n])
                    cp.start() if go else cp.wait()

    @pl.when(i == 0)
    def _():
        cp = pltpu.make_async_copy(h_ref.at[:, pl.ds(pl.multiple_of(me * nr, 128), nr)], hbuf, sem.at[2, 0])
        cp.start()
        fetch(0, 0, True)
        cp.wait()
        hT[...] = hbuf[...].T
    slot = i % 2

    @pl.when(i + 1 < last)
    def _(): fetch(i + 1, 1 - slot, True)
    fetch(i, slot, False)
    nq = nk // 2

    def put(j, slot, go):
        def one(ref, n, cond):
            @pl.when(cond)
            def _():
                cp = pltpu.make_async_copy(stage.at[slot], ref.at[:, pl.ds(pl.multiple_of(n * nk, nk), nk), :], sem.at[2, slot + 1])
                cp.start() if go else cp.wait()
        one(q_ref, jnp.minimum(j, nq - 1), j < nq)
        one(k_ref, 0, j == nq)
        one(v_ref, 0, j == nq + 1)

    @pl.when(i >= 2)
    def _(): put(i - 2, slot, False)
    stage[slot] = jnp.dot(hT[...], rhs[slot], preferred_element_type=F32).reshape(stage.shape[1:])
    put(i, slot, True)

    @pl.when(i == last - 1)
    def _():
        put(i - 1, 1 - slot, False)
        put(i, slot, False)


def dw_call(h, d, kv):
    nb, nk, seq, dc = d.shape
    t, w = h.shape
    nr = w // kv
    hd = dc // 6
    nq = nk // 2
    return pl.pallas_call(functools.partial(dw_kernel, 4), grid=(nq + 2,), in_specs=[ANY, ANY], out_specs=[ANY] * 3,
                          out_shape=[sds((nr, nq * nk, hd), F32)] + [sds((nr, nk, hd), F32)] * 2,
                          scratch_shapes=[V((nr, t), BF), V((t, nr), BF), V((2, t, nk * hd), BF), V((2, nr, nk, hd), F32), DS((3, nb * nk))], compiler_params=params(), name='dw')(h, d)


def dh_kernel(nt, parts, d_ref, *refs):
    w_refs, (x_any, dy_any, g_ref, dx_ref, s_ref, lhs, dh, x_ref, dy_ref, sem) = refs[:parts], refs[parts:]
    nb, nk, seq, dc = d_ref.shape
    me = lax.axis_index('cp')
    m = lhs.shape[0]
    bt = m // nb
    i = pl.program_id(0)
    tn = w_refs[0].shape[1]
    late = [pltpu.make_async_copy(x_any, x_ref, sem.at[nb * nk]), pltpu.make_async_copy(dy_any, dy_ref, sem.at[nb * nk + 1])]

    @pl.when(i == 0)
    def _():
        cps = [pltpu.make_async_copy(d_ref.at[b, n, pl.ds(pl.multiple_of(me * bt, bt), bt), :], lhs.at[b * bt:(b + 1) * bt, n * dc:(n + 1) * dc], sem.at[b * nk + n]) for b in range(nb) for n in range(nk)]
        for cp in cps + late: cp.start()
        for cp in cps: cp.wait()

    @pl.when(i < nt)
    def _():
        w = jnp.concatenate([r[k] for r in w_refs for k in range(r.shape[0])], axis=1)
        dh[jnp.minimum(i, nt - 1)] = lax.dot_general(lhs[...], w, NT, preferred_element_type=F32)

    @pl.when(i == nt)
    def _():
        for cp in late: cp.wait()
        s_ref[...] = jnp.zeros_like(s_ref)
        rc = 32
        sub = s_ref.shape[0] // 2
        fold = lambda v: v.reshape(rc // sub, sub, -1).sum(0)

        def body(r, _):
            rr = pl.ds(pl.multiple_of(r * rc, rc), rc)
            x_hat, inv = ln_stats(x_ref[rr, :].astype(F32))
            g = jnp.concatenate([dh[k, rr, :] for k in range(nt)], axis=1)
            gh = g * (1.0 + g_ref[...])
            m1 = jnp.mean(gh, axis=-1, keepdims=True)
            m2 = jnp.mean(gh * x_hat, axis=-1, keepdims=True)
            dx_ref[rr, :] = (dy_ref[rr, :].astype(F32) + inv * (gh - m1 - x_hat * m2)).astype(BF)
            s_ref[0:sub, :] += fold(g * x_hat)
            s_ref[sub:, :] += fold(g)
            return 0
        lax.fori_loop(0, m // rc, body, 0)


def dh_call(d, w2, x, dy, gain, tn=512, parts=3):
    nb, nk, seq, dc = d.shape
    nw, w, tw = w2.shape
    m = x.shape[0]
    nt = w // tn
    wspec = lambda p: pl.BlockSpec((nw // parts, tn, tw), lambda i: (p, jnp.minimum(i, nt - 1), 0))
    return pl.pallas_call(functools.partial(dh_kernel, nt, parts), grid=(nt + 1,), in_specs=[ANY] + [wspec(p) for p in range(parts)] + [ANY, ANY, pl.BlockSpec((1, w), lambda i: (0, 0))],
                          out_specs=[pl.BlockSpec((m, w), lambda i: (0, 0)), pl.BlockSpec((16, w), lambda i: (0, 0))], out_shape=[sds((m, w), BF), sds((16, w), F32)],
                          scratch_shapes=[V((m, nk * dc), BF), V((nt, m, tn), F32), V((m, w), BF), V((m, w), BF), DS((nb * nk + 2,))], compiler_params=params(), name='dh')(d, *[w2] * parts, x, dy, gain[None])


def sum_kernel(ncp, s_ref, o_ref, own, buf, send, recv):
    me = lax.axis_index('cp')
    M = pl.DeviceIdType.MESH
    sub = s_ref.shape[0] // 2
    barrier = pltpu.get_barrier_semaphore()
    for k in range(1, ncp): pl.semaphore_signal(barrier, inc=1, device_id={'cp': (me + k) % ncp}, device_id_type=M)
    for r in (0, 1): own[r:r + 1, :] = jnp.sum(s_ref[r * sub:(r + 1) * sub, :], axis=0, keepdims=True)
    pl.semaphore_wait(barrier, ncp - 1)
    cps = [pltpu.make_async_remote_copy(src_ref=own, dst_ref=buf.at[k], send_sem=send.at[k], recv_sem=recv.at[k], device_id={'cp': (me + k) % ncp}, device_id_type=M) for k in range(1, ncp)]
    for cp in cps: cp.start()
    buf[0] = own[...]
    for cp in cps: cp.wait()
    tot = buf[me]
    for dev in range(1, ncp): tot = tot + buf[(me + ncp - dev) % ncp]
    o_ref[...] = tot


def sum_call(s, ncp, cid):
    full = pl.BlockSpec(memory_space=pltpu.VMEM)
    w = s.shape[1]
    return pl.pallas_call(functools.partial(sum_kernel, ncp), in_specs=[full], out_specs=full, out_shape=sds((2, w), F32),
                          scratch_shapes=[V((2, w), F32), V((ncp, 2, w), F32), DS((ncp,)), DS((ncp,))], compiler_params=pltpu.CompilerParams(collective_id=cid, has_side_effects=True), name='sums')(s)


MASK = -1e30
HD, GQ, QB, HALF = 128, 4, 128, 64
ROT = HALF // 2
QW = GQ * HD
TW = 2 * HD
NCH = 4
UT = 3
SLOTS, RSLOTS = 3, 10
CHUNK = 2
MESH = pl.DeviceIdType.MESH


def rot(x, c, s):
    lane = lax.broadcasted_iota(jnp.int32, x.shape, 1)
    return x * c + jnp.where(lane < ROT, pltpu.roll(x, HD - ROT, 1), pltpu.roll(x, ROT, 1)) * s


def dot(a, b): return jnp.dot(a, b, preferred_element_type=F32)


def ntdot(a, b): return lax.dot_general(a, b, NT, preferred_element_type=F32)


def att_scores(i, q_ref, k_ref, v_ref, da_ref):
    L = QB * (i + 1)
    stack = lambda ref: jnp.concatenate([ref[L - QB:L, HD * h:HD * h + HD] for h in range(GQ)], axis=0)
    q4, da4 = stack(q_ref), stack(da_ref)
    return q4, da4, ntdot(k_ref[0:L, :], q4), ntdot(v_ref[0:L, :], da4)


def att_probs(i, q4, da4, sT, dpT):
    L, scale = QB * (i + 1), HD ** -0.5
    kr = lax.broadcasted_iota(jnp.int32, (QB, GQ * QB), 0)
    qc = lax.broadcasted_iota(jnp.int32, (QB, GQ * QB), 1) & (QB - 1)
    diag = jnp.where(kr <= qc, sT[L - QB:L, :], MASK)
    sT = jnp.concatenate([sT[:L - QB, :], diag], axis=0) if i else diag
    e = jnp.exp2((sT - jnp.max(sT, axis=0, keepdims=True)) * (scale * math.log2(math.e)))
    p = e * (1.0 / jnp.sum(e, axis=0, keepdims=True))
    ds = (p * (dpT - jnp.sum(p * dpT, axis=0, keepdims=True)) * scale).astype(BF)
    return q4, da4, p.astype(BF), ds


def att_store(i, kT, vT, rope, a_ref, d_ref, dk_acc, dv_acc, q4, da4, pb, ds):
    L = QB * (i + 1)
    r, full, head = slice(L - QB, L), slice(0, L), lambda h: slice(HD * h, HD * h + HD)
    aT = dot(vT[:, full], pb)
    for h in range(GQ): a_ref[r, head(h)] = aT[:, head(h)].T.astype(BF)
    dv_acc[full, :] += dot(pb, da4)
    dk_acc[full, :] += dot(ds, q4)
    dqT = dot(kT[:, full], ds)
    c, s = rope[0, r, :], -rope[1, r, :]
    for h in range(GQ): d_ref[r, head(h)] = rot(dqT[:, head(h)].T, c, s).astype(BF)


def kg_kernel(nchip, owned, plan, h_own, dy_own, cs_own, wq, wk, wv, wo,
              h_all, dy_all, w2, a_own, a4, dqkv, cs_all, q_hbm, k_hbm, v_hbm, da_hbm, a_tmp,
              lhs, rope, wt, wot,
              send, recv, csend, crecv, wsend, wrecv, rsend, rrecv, osend, orecv, asend, arecv, fsend, frecv,
              lsem, wsem, osem, isem, iosem, aisem, aosem, ownsem, bsem):
    nb, bt, width = h_own.shape
    nkv = w2.shape[0] // UT
    T = q_hbm.shape[2]
    nloc = nkv // 2
    cb = 2 * bt
    me = lax.axis_index('cp')
    chip, core = me // 2, me % 2
    at = lambda step, c=core: 2 * ((chip + step) % nchip) + c
    right, left, opp, part = at(1), at(nchip - 1), at(2), 2 * chip + 1 - core
    other = 1 - core
    own_t, all_t = (h_own, dy_own), (h_all, dy_all)
    ds = lambda i, n: pl.ds(pl.multiple_of(i * n, n), n)
    blk = lambda a: ds(a, bt)

    barrier = pltpu.get_barrier_semaphore()
    ncp = 2 * nchip
    for k in range(1, ncp): pl.semaphore_signal(barrier, inc=1, device_id={'cp': (me + k) % ncp}, device_id_type=MESH)
    pl.semaphore_wait(barrier, ncp - 1)

    def remote(src, dst, s, r, dev):
        return pltpu.make_async_remote_copy(src_ref=src, dst_ref=dst, send_sem=s, recv_sem=r, device_id={'cp': dev}, device_id_type=MESH)

    local = pltpu.make_async_copy
    pending = []

    def go(make, *ar):
        make(*ar).start()
        pending.append((make, ar))

    def ring(view, own, ss, rs, half):
        def copy(ch, src, slot, dev, lo=0, n=2 * half): return remote(src if src is not None else view(slot, lo, n), view(slot, lo, n), ss.at[ch], rs.at[ch], dev)

        def D():
            for ch, dev in enumerate((right, left, part)): go(copy, ch, own, me, dev)

        def got(ch, slot, lo=0, n=2 * half): copy(ch, None, slot, part, lo, n).wait_recv()

        def Fw():
            got(0, left)
            go(copy, 3, None, left, right, 0, half)
            got(1, right)
            go(copy, 4, None, right, left, half, half)
            go(copy, 5, None, left, part)
            go(copy, 6, None, right, part)

        def G():
            got(3, opp, 0, half)
            got(4, opp, half, half)
            go(copy, 7, None, opp, part)

        def ready(pos):
            if pos == 0: got(2, part)
            if pos == 1: got(6, at(1, other))
            if pos == 2: got(5, at(nchip - 1, other))
            if pos == 3: got(7, at(2, other))
        return D, Fw, G, ready

    rings = []
    for t in range(2 * nb):
        b, kind = t // 2, t % 2
        view = lambda slot, lo, n, b=b, kind=kind: all_t[kind].at[b, pl.ds(pl.multiple_of(slot * bt + lo, bt // 2), n), :]
        rings.append(ring(view, own_t[kind].at[b], send.at[t], recv.at[t], bt // 2))
    oview = lambda slot, lo, n: dqkv.at[owned, slot, pl.ds(lo, n), :]
    rings.append(ring(oview, dqkv.at[owned, me], osend, orecv, q_hbm.shape[2] // 2))

    def cs_copy(b, ch, src, slot, dev): return remote(src, cs_all.at[b, blk(slot), :], csend.at[b, ch], crecv.at[b, ch], dev)

    def cs_send(b):
        for ch, dev in enumerate((right, opp, left, part)): go(cs_copy, b, ch, cs_own.at[b], me, dev)

    def cs_forward(b):
        for ch, slot in enumerate((left, opp, right)):
            cs_copy(b, ch, cs_own.at[b], slot, part).wait_recv()
            go(cs_copy, b, 4 + ch, cs_all.at[b, blk(slot), :], slot, part)

    def cs_ready(b):
        cs_copy(b, 3, cs_own.at[b], part, part).wait_recv()
        for ch, step in enumerate((nchip - 1, 2, 1)): cs_copy(b, 4 + ch, cs_own.at[b], at(step, other), part).wait_recv()

        def scope(cst):
            for dev in range(ncp):
                @pl.when(dev != me)
                def _(): local(cs_all.at[b, dev * bt:(dev + 1) * bt, :], cst.at[dev * bt:(dev + 1) * bt, :], bsem.at[dev]).start()
            local(cs_own.at[b], cst.at[blk(me), :], bsem.at[me]).start()
            for dev in range(ncp): local(cs_own.at[b], cst.at[dev * bt:(dev + 1) * bt, :], bsem.at[dev]).wait()
            packed = cst[...]
            turned = lax.broadcasted_iota(jnp.int32, packed.shape, 1) < HALF
            rope[b, 0] = jnp.where(turned, packed, 1.0)
            rope[b, 1] = jnp.where(turned, pltpu.roll(packed, HALF, 1), 0.0)
        pl.run_scoped(scope, V((T, HD), F32))

    STEP = (0, 1, nchip - 1, 2)
    crow = lambda pos: ds((chip + STEP[pos]) % nchip, cb)

    def loads(t, pos):
        b, kind = t // 2, t % 2
        if pos == 0:
            return [local(own_t[kind].at[b], lhs.at[kind, blk(core), :], lsem.at[kind, 0]), local(all_t[kind].at[b, blk(part), :], lhs.at[kind, blk(other), :], lsem.at[kind, nchip])]
        return [local(all_t[kind].at[b, crow(pos), :], lhs.at[kind, pl.ds(pos * cb, cb), :], lsem.at[kind, pos])]

    def own_back(t): return local(lhs.at[t % 2, blk(core), :], all_t[t % 2].at[t // 2, blk(me), :], ownsem.at[t % 2])

    def load(t, pos_list):
        for pos in pos_list:
            rings[t][3](pos)
            for cp in loads(t, pos): cp.start()

    def key_head(b, i): return me if b == owned else 2 * mine(i // 2) + i % 2

    primed = set()

    def tiles(t, pos_list, per, buf, start, wait, compute, dst, mid):
        b, kind = t // 2, t % 2
        m0, m = pos_list[0] * cb, len(pos_list) * cb
        cnt = per * (1 if b == owned else nloc)
        tid = lambda x: per * key_head(b, x // per) + x % per

        def scope(ost):
            prime(t)
            primed.discard(t)
            for pos in pos_list:
                for cp in loads(t, pos): cp.wait()
            if pos_list[0] == 0: own_back(t).start()

            def stores(x, slot, start_it):
                for y, pos in enumerate(pos_list):
                    dst(b, x // per, x % per, crow(pos), ost.at[slot, pl.ds(y * cb, cb), :], slot, y, start_it)

            def body(x, _):
                for when, ops in mid.items():
                    @pl.when(x == when)
                    def _():
                        for op, *ar in ops: ACT[op](*ar)
                slot, ws = x % 2, x % SLOTS
                wait(tid(x), buf, ws)

                @pl.when(x >= 1)
                def _():
                    @pl.when(x + SLOTS - 1 < cnt)
                    def _(): start(tid(x + SLOTS - 1), buf, (x + SLOTS - 1) % SLOTS)

                @pl.when(x >= 2)
                def _(): stores(x - 2, slot, False)
                compute(b, x % per, lambda r, n: lhs[kind, m0 + r:m0 + r + n, :], buf.at[ws], ost, slot, pos_list)
                stores(x, slot, True)
                return 0
            lax.fori_loop(0, cnt, body, 0)
            for x in (cnt - 2, cnt - 1): stores(x, x % 2, False)
            if pos_list[0] == 0: own_back(t).wait()
        pl.run_scoped(scope, V((2, m, TW), BF))

    def run(cp, start_it): cp.start() if start_it else cp.wait()

    def w_start(n, buf, slot):
        c = width // NCH
        for y in range(NCH): local(w2.at[n, pl.ds(y * c, c), :], buf.at[slot, pl.ds(y * c, c), :], wsem.at[0, slot]).start()

    def w_wait(n, buf, slot): local(w2.at[n], buf.at[slot], wsem.at[0, slot]).wait()

    def qkv_dst(b, i, u, rr, src, slot, y, start_it):
        @pl.when(u < 2)
        def _(): run(local(src, q_hbm.at[b, i, rr, ds(jnp.minimum(u, 1), TW)], osem.at[slot, y]), start_it)

        @pl.when(u == 2)
        def _():
            run(local(src.at[:, 0:HD], k_hbm.at[b, i, rr, :], osem.at[slot, y]), start_it)
            run(local(src.at[:, HD:TW], v_hbm.at[b, i, rr, :], osem.at[slot, nchip + y]), start_it)

    def qkv_compute(b, u, left, w, ost, slot, pos_list):
        for y0 in range(0, len(pos_list), CHUNK):
            part_list = pos_list[y0:y0 + CHUNK]
            res = dot(left(y0 * cb, len(part_list) * cb), w[...])
            for y, pos in enumerate(part_list):
                c, s = rope[b, 0, crow(pos), :], rope[b, 1, crow(pos), :]
                rr, ro = slice(y * cb, (y + 1) * cb), slice((y0 + y) * cb, (y0 + y + 1) * cb)
                ost[slot, ro, 0:HD] = rot(res[rr, 0:HD], c, s).astype(BF)
                ost[slot, ro, HD:TW] = jnp.where(u == 2, res[rr, HD:TW], rot(res[rr, HD:TW], c, s)).astype(BF)

    def qkv(b, pos_list, mid={}): tiles(2 * b, pos_list, UT, wt, w_start, w_wait, qkv_compute, qkv_dst, mid)

    def o_start(n, buf, slot):
        c = TW // NCH
        for y in range(NCH): local(wo.at[ds(n * NCH + y, c), :], buf.at[slot, pl.ds(y * c, c), :], wsem.at[1, slot]).start()

    def o_wait(n, buf, slot): local(wo.at[ds(n, TW), :], buf.at[slot], wsem.at[1, slot]).wait()

    def da_dst(b, i, u, rr, src, slot, y, start_it): run(local(src, da_hbm.at[b, i, rr, ds(u, TW)], osem.at[slot, y]), start_it)

    def da_compute(b, u, left, w, ost, slot, pos_list):
        for y0 in range(0, len(pos_list), CHUNK):
            n = min(CHUNK, len(pos_list) - y0) * cb
            ost[slot, y0 * cb:y0 * cb + n, :] = ntdot(left(y0 * cb, n), w[...]).astype(BF)

    def da(b, pos_list, mid={}): tiles(2 * b + 1, pos_list, 2, wot, o_start, o_wait, da_compute, da_dst, mid)

    def prime(t):
        if t in primed: return
        primed.add(t)
        b, per, buf, start = t // 2, (UT, 2)[t % 2], (wt, wot)[t % 2], (w_start, o_start)[t % 2]
        for x in range(min(per * (1 if b == owned else nloc), SLOTS)): start(per * key_head(b, x // per) + x % per, buf, x)

    OCT = nkv

    def rl(src_of, dst_of, nblk):
        def scope(wst, wrl):
            for i in range(RSLOTS): src_of(i, wst.at[i], i).start()

            def body(j, _):
                for u in range(RSLOTS):
                    i, slot = RSLOTS * j + u, u % 2
                    src_of(i, wst.at[u], u).wait()

                    @pl.when(i >= 2)
                    def _():
                        for cp in dst_of(i - 2, wrl.at[slot], slot): cp.wait()
                    wrl[slot] = wst[u].reshape(RB, OCT * HD)
                    for cp in dst_of(i, wrl.at[slot], slot): cp.start()

                    @pl.when(i + RSLOTS < nblk)
                    def _(): src_of(i + RSLOTS, wst.at[u], u).start()
                return 0
            lax.fori_loop(0, nblk // RSLOTS, body, 0)
            for slot in (0, 1):
                for cp in dst_of(nblk - 2 + slot, wrl.at[slot], slot): cp.wait()
        pl.run_scoped(scope, V((RSLOTS, RB, OCT, HD), BF), V((2, RB, OCT * HD), BF))

    half_w = width // 2
    mine = lambda t: t * 2 + core
    theirs = lambda t: t * 2 + other

    def q_tile(octet, x): return UT * (2 * octet + x // 2) + x % 2

    def w_copy(ch, tile, rows): return remote(w2.at[tile, rows, :], w2.at[tile, rows, :], wsend.at[ch], wrecv.at[ch], part)

    def rl_q(t):
        rl(lambda i, buf, slot: local(wq.at[ds(i, RB), ds(mine(t), OCT), :], buf, isem.at[slot]),
           lambda i, buf, slot: [local(buf.at[:, pl.ds(TW * x, TW)], w2.at[q_tile(mine(t), x), ds(i, RB), :], iosem.at[slot, x]) for x in range(NCH)], width // RB)

    def q_copy(t, x): return w_copy(t * NCH + x, q_tile(mine(t), x), pl.ds(0, width))

    def q_send(t):
        for x in range(NCH): go(q_copy, t, x)

    def rl_kv(kv):
        w = (wk, wv)[kv]
        base = half_w // RB
        rl(lambda i, buf, slot: local(w.at[ds(core * base + i, RB)], buf, isem.at[slot]),
           lambda i, buf, slot: [local(buf.at[:, pl.ds(n * HD, HD)], w2.at[UT * n + 2, ds(core * base + i, RB), kv * HD:(kv + 1) * HD], iosem.at[slot, n]) for n in range(nkv)], base)
        if kv:
            for n in range(nkv): go(w_copy, 2 * NCH + n, UT * n + 2, ds(core, half_w))

    def wq_ready():
        for t in (0, 1):
            for x in range(NCH): w_copy(t * NCH + x, q_tile(theirs(t), x), pl.ds(0, width)).wait_recv()

    def wkv_ready():
        for n in range(nkv): w_copy(2 * NCH + n, UT * n + 2, ds(other, half_w)).wait_recv()

    def att_ins(b, i, slot, bufs): return [local(src.at[b, i], dst.at[slot], aisem.at[slot, x]) for x, (src, dst) in enumerate(zip((q_hbm, k_hbm, v_hbm, da_hbm), bufs))]

    def att_outs(b, i, slot, out_a, out_d):
        n = key_head(b, i)
        return [local(out_a.at[slot], a_tmp.at[b, i], aosem.at[slot, 0]), local(out_d.at[slot], dqkv.at[b, n], aosem.at[slot, 1]), local(out_a.at[slot, blk(me), :], a_own.at[b, n], aosem.at[slot, 2])]

    def keep(b, i, slot, out_a, start_it):
        @pl.when(key_head(b, i) == me)
        def _(): run(local(out_a.at[slot], a4.at[b], aosem.at[slot, 3]), start_it)

    whole = [b for b in range(nb) if b != owned]

    def pair_copies(b, i, n):
        f = whole.index(b)
        return [remote(dqkv.at[b, n], dqkv.at[b, n], rsend.at[f, i, 0], rrecv.at[f, i, 0], part),
                remote(a_tmp.at[b, i, blk(part), :], a_own.at[b, n], rsend.at[f, i, 1], rrecv.at[f, i, 1], part)]

    def four_copy(b, i): return remote(a_tmp.at[b, i], a4.at[b], fsend.at[whole.index(b)], frecv.at[whole.index(b)], part)

    def att(b):
        cnt = 1 if b == owned else nloc

        def scope(in_q, in_k, in_v, in_da, out_a, out_d, dk_acc, dv_acc, kT, vT):
            bufs = (in_q, in_k, in_v, in_da)
            for cp in att_ins(b, 0, 0, bufs): cp.start()

            def done(i, slot):
                for cp in att_outs(b, i, slot, out_a, out_d): cp.wait()
                keep(b, i, slot, out_a, False)
                if b != owned:
                    for cp in pair_copies(b, i, key_head(b, i)): cp.start()

                    @pl.when(key_head(b, i) == part)
                    def _(): four_copy(b, i).start()

            def body(i, _):
                slot = i % 2
                for cp in att_ins(b, i, slot, bufs): cp.wait()

                @pl.when(i + 1 < cnt)
                def _():
                    for cp in att_ins(b, i + 1, 1 - slot, bufs): cp.start()

                @pl.when(i >= 2)
                def _(): done(i - 2, slot)
                hook(b, i)
                q, k, v, g = (r.at[slot] for r in bufs)
                dk_acc[...] = jnp.zeros_like(dk_acc)
                dv_acc[...] = jnp.zeros_like(dv_acc)
                kT[...] = k[...].T
                vT[...] = v[...].T
                nblk = T // QB
                scores = att_scores(0, q, k, v, g)
                for x in range(nblk):
                    following = att_scores(x + 1, q, k, v, g) if x + 1 < nblk else None
                    att_store(x, kT, vT, rope.at[b], out_a.at[slot], out_d.at[slot], dk_acc, dv_acc, *att_probs(x, *scores))
                    scores = following
                out_d[slot, :, QW:QW + HD] = rot(dk_acc[...], rope[b, 0], -rope[b, 1]).astype(BF)
                out_d[slot, :, QW + HD:] = dv_acc[...].astype(BF)
                for cp in att_outs(b, i, slot, out_a, out_d): cp.start()
                keep(b, i, slot, out_a, True)
                return 0
            lax.fori_loop(0, cnt, body, 0)
            for i in range(max(cnt - 2, 0), cnt): done(i, i % 2)
        two = lambda w: V((2, T, w), BF)
        pl.run_scoped(scope, two(QW), two(HD), two(HD), two(QW), two(QW), two(QW + TW), V((T, HD), F32), V((T, HD), F32), V((HD, T), BF), V((HD, T), BF))

    hooks = {}

    def hook(b, i):
        for j, ops in hooks.get(b, {}).items():
            @pl.when(i == j)
            def _():
                for op, *ar in ops: ACT[op](*ar)

    def a_copy(k, src, slot, dev): return remote(src, a_own.at[owned, slot], asend.at[k], arecv.at[k], dev)

    def a_send():
        for k in range(1, ncp): go(a_copy, k, a_tmp.at[owned, 0, blk((me + k) % ncp), :], me, (me + k) % ncp)

    def all_in():
        for k in range(1, ncp): a_copy(k, a_tmp.at[owned, 0, blk(me), :], (me + ncp - k) % ncp, part).wait_recv()
        for b in whole:
            for i in range(nloc):
                for cp in pair_copies(b, i, key_head(b, i)): cp.wait_send()
                for cp in pair_copies(b, i, 2 * theirs(i // 2) + i % 2): cp.wait_recv()

            @pl.when(chip % 2 == core)
            def _(): four_copy(b, 0).wait_send()

            @pl.when(chip % 2 != core)
            def _(): four_copy(b, 0).wait_recv()

    ACT = {'L0': lambda t, ps: [cp.start() for p in ps for cp in loads(t, p)], 'T': cs_send, 'TF': cs_forward, 'TR': cs_ready, 'D': lambda t: rings[t][0](), 'F': lambda t: rings[t][1](), 'G': lambda t: rings[t][2](), 'N': lambda t, ps: [rings[t][3](p) for p in ps],
           'L': load, 'RQ': rl_q, 'SQ': q_send, 'RK': rl_kv, 'WQ': wq_ready, 'WK': wkv_ready, 'Q': qkv, 'O': da, 'AS': a_send, 'IN': all_in, 'H': lambda b, j, ops: hooks.setdefault(b, {}).update({j: ops}), 'A': att}
    tensor = lambda op, b, *ar: 2 * b + (op == 'O')
    for j, (op, *ar) in enumerate(plan):
        if op in ('Q', 'O', 'A'):
            later = [o for o in plan[j + 1:] if o[0] in ('Q', 'O')][:1]
            for o in later:
                if o[0] != op and (op == 'A' or o[:2] != ('Q', owned)): prime(tensor(*o))
        ACT[op](*ar)
    for make, ar in pending: make(*ar).wait_send()


S0, S1, S2, S3, S4, S5, S6, S7, S8, S9, S10 = range(11)
NEAR, FAR, EACH, HERE, AWAY = (S0, S1, S2), (S3,), (S0, S1, S2, S3), (S0,), (S1, S2, S3)
PLAN = [('T', S0), ('D', S0), ('D', S1), ('T', S1), ('T', S2), ('RK', S0), ('RK', S1), ('RQ', S0), ('TF', S0), ('F', S0), ('D', S2), ('RQ', S1), ('TR', S0), ('L', S0, NEAR), ('WK',),
        ('Q', S0, NEAR, {S2: [('SQ', S0)], S6: [('F', S1), ('D', S3)], S10: [('L', S1, NEAR)]}), ('G', S0), ('L', S0, FAR), ('SQ', S1), ('O', S0, NEAR), ('TF', S1), ('TF', S2), ('Q', S0, FAR),
        ('F', S2), ('D', S4), ('G', S1), ('L', S1, FAR), ('TR', S1), ('TR', S2), ('L', S2, NEAR), ('O', S0, FAR),
        ('H', S0, S1, [('F', S3), ('D', S5)]), ('H', S0, S2, [('L', S3, NEAR), ('G', S2), ('L', S2, FAR)]), ('WQ',), ('A', S0),
        ('Q', S1, EACH), ('L', S4, HERE), ('F', S4), ('Q', S2, HERE), ('G', S3), ('L', S3, FAR), ('L', S4, NEAR[S1:]), ('O', S1, EACH), ('L', S5, HERE), ('A', S1),
        ('F', S5), ('D', S6), ('AS',), ('G', S4), ('L', S4, FAR), ('L', S5, NEAR[S1:]), ('Q', S2, AWAY, {S9: [('G', S5), ('L', S5, FAR)]}), ('O', S2, EACH), ('H', S2, S1, [('F', S6)]), ('H', S2, S3, [('G', S6)]), ('A', S2), ('N', S6, EACH), ('IN',)]
RB = 128


def kg_call(h_own, dy_own, cs_own, wq, wk, wv, wo, ncp, owned=1, plan=None):
    nb, bt, width = h_own.shape
    T = bt * ncp
    nkv = wk.shape[1]
    nloc = nkv // 2
    seqs = lambda *s: sds((nb,) + s, BF)
    outs = [seqs(T, width)] * 2 + [sds((UT * nkv, width, TW), BF), seqs(nkv, bt, QW), seqs(T, QW), seqs(nkv, T, QW + TW), sds((nb, T, HD), F32),
            seqs(nloc, T, QW), seqs(nloc, T, HD), seqs(nloc, T, HD), seqs(nloc, T, QW), seqs(nloc, T, QW)]
    two = lambda *s: [DS(s), DS(s)]
    scratch = [V((2, T, width), BF), V((nb, 2, T, HD), F32), V((SLOTS, width, TW), BF), V((SLOTS, TW, width), BF)] + two(2 * nb, 8) + two(nb, 7) + two(2 * NCH + nkv) + two(nb - 1, nloc, 2) + two(8) + two(ncp) + two(nb - 1)
    scratch += [DS((2, 5)), DS((2, SLOTS)), DS((2, 8)), DS((RSLOTS,)), DS((2, 8)), DS((2, 4)), DS((2, 4)), DS((2,)), DS((ncp,))]
    return pl.pallas_call(functools.partial(kg_kernel, ncp // 2, owned, plan or PLAN), out_shape=outs, in_specs=[ANY] * 7, out_specs=[ANY] * len(outs), scratch_shapes=scratch,
                          compiler_params=params(collective_id=0, has_side_effects=True), name='gather')(h_own, dy_own, cs_own, wq, wk, wv, wo)


ROPE_BASE = 10000.0


def rope_table(positions):
    freq_tab = jnp.exp(jnp.arange(ROT, dtype=F32) * (-2.0 * math.log(ROPE_BASE) / HALF))
    angles = positions.astype(F32)[..., None] * freq_tab
    cos, sin = jnp.cos(angles), jnp.sin(angles)
    return jnp.concatenate([cos, cos, -sin, sin], -1)


def solution(mesh):
    ncp = mesh.shape['cp']

    def device_step(x_act, d_out, positions, ln_gain, ln_bias, w_query, w_key, w_value, w_out):
        nb, bt, width = x_act.shape
        flat = lambda v: v.reshape(nb * v.shape[1], v.shape[2])
        x, dy = flat(x_act), flat(d_out)
        h = norm_call(x, ln_gain, ln_bias).reshape(x_act.shape)
        h_all, dy_all, w2, a_own, a4, dqkv = kg_call(h, d_out, rope_table(positions), w_query, w_key, w_value, w_out, ncp)[:6]
        dx, sums = dh_call(dqkv, w2, x, dy, ln_gain)
        sums = sum_call(sums, ncp, 1)
        block_out = out_call(a_own, w_out, x)
        dwo = dwo_call(flat(a4), flat(dy_all))
        dwq, dwk, dwv = dw_call(flat(h_all), dqkv, ncp)
        return (block_out.reshape(x_act.shape), dx.reshape(x_act.shape), dwq, dwk, dwv, dwo, sums[0], sums[1])

    row, rep = P('dp', 'cp', None), P(None)
    wrow = P(('dp', 'cp'), None, None)
    return jax.shard_map(device_step, mesh=mesh, in_specs=(row, row, P('dp', 'cp'), rep, rep, rep, rep, rep, rep),
                         out_specs=(row, row, wrow, wrow, wrow, P(('dp', 'cp'), None), P('dp'), P('dp')), check_vma=False)
```
